256 devices in a mesh: gx: 4 (over x), gy: 8 (over y, core), ha: 8 (over z).
Axes of the slice: x: 4, y: 4, z: 8, core: 2. Of those that a mesh axis runs over, the one named last changes fastest.
Arguments:
- level_set: float32 [32, 128, 80, 128], P('gx', 'gy', 'ha'), may hold values from -4 to 4
- wind_field: float32 [2, 32, 128], P(None, 'gx', 'gy'), may hold values from -3 to 3
Outputs:
- increment: float32 [32, 128, 80, 128], P('gx', 'gy', 'ha')
The draws below stay inside these ranges and needn't reach their ends.
All inputs are finite; a program needn't handle non-finite values.
Results may differ from the reference program's by a relative error of at most 0.000073.
Values sent between devices are 32-bit elements; how exact they have to be, the bound alone decides.
No kernel may reach another device: no remote copies, remote signals or barrier semaphores. Data moves between devices by JAX's collectives and lax.ppermute only.
A program may use at most 128 MiB of HBM per device.

```python
import math
import jax
import jax.numpy as jnp
from jax import lax

NV = 128
NX = 32
NY = 128
NH = 80


CELL_SIZE = 0.05


def draw_level_set(key, part):
    rough_key = jax.random.fold_in(key, 11)
    center_key = jax.random.fold_in(key, 12)
    shape = (NX, NY, NH, NV)
    centers = jax.random.uniform(center_key, (2,), jnp.float32, 0.3, 0.7)
    pos_x = (jnp.arange(NX, dtype=jnp.float32) + 0.5) / NX
    pos_y = (jnp.arange(NY, dtype=jnp.float32) + 0.5) / NY
    span_x = (pos_x - centers[0]) * NX * CELL_SIZE
    span_y = (pos_y - centers[1]) * NY * CELL_SIZE
    smooth = jnp.sqrt(span_x[:, None] ** 2 + span_y[None, :] ** 2 + 0.01) - 0.25 * NX * CELL_SIZE
    smooth = smooth[:, :, None, None]
    rough = 0.5 * jax.random.normal(rough_key, shape, jnp.float32)
    surface = rough + smooth
    return jnp.clip(surface, -4.0, 4.0)


def draw_wind_field(key, part):
    raw_key = jax.random.fold_in(key, 21)
    shape = (2, NX, NY)
    ramp = 0.1 + 2.9 * (jnp.arange(NX, dtype=jnp.float32) + 0.5) / NX
    raw = jax.random.uniform(raw_key, shape, jnp.float32, -1.0, 1.0)
    return raw * ramp[None, :, None]


def setup_inputs(seed: int = 0) -> dict:
    streams_of = jax.random.split(jax.random.key(seed), 3)
    return {
        "level_set": draw_level_set(jax.random.fold_in(streams_of[2], 71), 0),
        "wind_field": draw_wind_field(jax.random.fold_in(streams_of[2], 71), 0),
    }


CELL_SIZE = 0.05
SPEED_LOW = 0.1
SPEED_SPAN = 0.4
TURN_MAX = 1.0
ACCEL_MAX = 0.05
CFL_NUMBER = 0.5
WENO_EPS = 1e-6


def ghost_rows(values, along, at_low):
    length = values.shape[along]
    if at_low:
        edge_row = lax.slice_in_dim(values, 0, 1, axis=along)
        next_row = lax.slice_in_dim(values, 1, 2, axis=along)
        reaches = (3.0, 2.0, 1.0)
    else:
        edge_row = lax.slice_in_dim(values, length - 1, length, axis=along)
        next_row = lax.slice_in_dim(values, length - 2, length - 1, axis=along)
        reaches = (1.0, 2.0, 3.0)
    slope_edge = edge_row - next_row
    return jnp.concatenate([edge_row + distance * slope_edge for distance in reaches], axis=along)


def extend(values, along):
    return jnp.concatenate([ghost_rows(values, along, True), values, ghost_rows(values, along, False)], axis=along)


def speed_shifts(values):
    length = values.shape[3]
    below_rows = ghost_rows(values, 3, True)
    above_rows = ghost_rows(values, 3, False)
    shifted = []
    for displace in range(-3, 4):
        pieces = []
        if displace < 0:
            pieces.append(lax.slice_in_dim(below_rows, 3 + displace, 3, axis=3))
        pieces.append(lax.slice_in_dim(values, max(displace, 0), length + min(displace, 0), axis=3))
        if displace > 0:
            pieces.append(lax.slice_in_dim(above_rows, 0, displace, axis=3))
        shifted.append(jnp.concatenate(pieces, axis=3) if len(pieces) > 1 else pieces[0])
    return shifted


def weno_side(left_far, left_near, middle, right_near, right_far):
    guess_one = left_far * (1.0 / 3.0) - left_near * (7.0 / 6.0) + middle * (11.0 / 6.0)
    guess_two = -left_near * (1.0 / 6.0) + middle * (5.0 / 6.0) + right_near * (1.0 / 3.0)
    guess_three = middle * (1.0 / 3.0) + right_near * (5.0 / 6.0) - right_far * (1.0 / 6.0)
    smooth_one = (13.0 / 12.0) * jnp.square(left_far - 2.0 * left_near + middle) + 0.25 * jnp.square(left_far - 4.0 * left_near + 3.0 * middle)
    smooth_two = (13.0 / 12.0) * jnp.square(left_near - 2.0 * middle + right_near) + 0.25 * jnp.square(left_near - right_near)
    smooth_three = (13.0 / 12.0) * jnp.square(middle - 2.0 * right_near + right_far) + 0.25 * jnp.square(3.0 * middle - 4.0 * right_near + right_far)
    weight_one = 0.1 / jnp.square(smooth_one + WENO_EPS)
    weight_two = 0.6 / jnp.square(smooth_two + WENO_EPS)
    weight_three = 0.3 / jnp.square(smooth_three + WENO_EPS)
    return (weight_one * guess_one + weight_two * guess_two + weight_three * guess_three) / (weight_one + weight_two + weight_three)


def weno_pair(shifted, spacing):
    slopes = [(shifted[position + 1] - shifted[position]) / spacing for position in range(6)]
    left_slope = weno_side(slopes[0], slopes[1], slopes[2], slopes[3], slopes[4])
    right_slope = weno_side(slopes[5], slopes[4], slopes[3], slopes[2], slopes[1])
    return left_slope, right_slope


def cell_rates(cos_head, sin_head, speeds, wind_x, wind_y, d_theta, d_speed):
    along_x = speeds[None, None, None, :] * cos_head[None, None, :, None] + wind_x[:, :, None, None]
    along_y = speeds[None, None, None, :] * sin_head[None, None, :, None] + wind_y[:, :, None, None]
    return jnp.abs(along_x) / CELL_SIZE + jnp.abs(along_y) / CELL_SIZE + TURN_MAX / d_theta + ACCEL_MAX / d_speed


def hamilton(x_pair, y_pair, head_pair, speed_pair, cos_head, sin_head, speeds, wind_x, wind_y):
    flow_x = speeds[None, None, None, :] * cos_head[None, None, :, None] + wind_x[:, :, None, None]
    flow_y = speeds[None, None, None, :] * sin_head[None, None, :, None] + wind_y[:, :, None, None]
    mean_x = 0.5 * (x_pair[0] + x_pair[1])
    mean_y = 0.5 * (y_pair[0] + y_pair[1])
    mean_head = 0.5 * (head_pair[0] + head_pair[1])
    mean_speed = 0.5 * (speed_pair[0] + speed_pair[1])
    value = -(flow_x * mean_x + flow_y * mean_y + TURN_MAX * jnp.abs(mean_head) + ACCEL_MAX * jnp.abs(mean_speed))
    damping = 0.5 * (jnp.abs(flow_x) * (x_pair[1] - x_pair[0]) + jnp.abs(flow_y) * (y_pair[1] - y_pair[0])
                     + TURN_MAX * (head_pair[1] - head_pair[0]) + ACCEL_MAX * (speed_pair[1] - speed_pair[0]))
    return -jnp.maximum(value - damping, 0.0)


def reference(level_set, wind_field):
    d_theta = 2.0 * math.pi / NH
    d_speed = SPEED_SPAN / NV
    angles = jnp.arange(NH, dtype=jnp.int32).astype(jnp.float32) * d_theta
    cos_head = jnp.cos(angles)
    sin_head = jnp.sin(angles)
    speeds = SPEED_LOW + SPEED_SPAN * (jnp.arange(NV, dtype=jnp.int32).astype(jnp.float32) + 0.5) / NV
    rows_all = jnp.arange(NX, dtype=jnp.int32)

    def plane_max(position):
        winds = lax.dynamic_slice_in_dim(wind_field, position, 1, 1)
        return jnp.max(cell_rates(cos_head, sin_head, speeds, winds[0], winds[1], d_theta, d_speed))

    time_step = CFL_NUMBER / jnp.max(lax.map(plane_max, rows_all))

    def advance(surface):
        x_padded = extend(surface, 0)

        def one_plane(position):
            x_plane = lax.dynamic_slice_in_dim(surface, position, 1, 0)
            x_shifted = [lax.dynamic_slice_in_dim(x_padded, position + 3 + displace, 1, 0) for displace in range(-3, 4)]
            y_padded = extend(x_plane, 1)
            y_shifted = [y_padded[:, 3 + displace:3 + displace + NY] for displace in range(-3, 4)]
            head_padded = jnp.concatenate([x_plane[:, :, NH - 3:], x_plane, x_plane[:, :, :3]], axis=2)
            head_shifted = [head_padded[:, :, 3 + displace:3 + displace + NH] for displace in range(-3, 4)]
            winds = lax.dynamic_slice_in_dim(wind_field, position, 1, 1)
            return hamilton(weno_pair(x_shifted, CELL_SIZE), weno_pair(y_shifted, CELL_SIZE),
                            weno_pair(head_shifted, d_theta), weno_pair(speed_shifts(x_plane), d_speed),
                            cos_head, sin_head, speeds, winds[0], winds[1])

        return lax.map(one_plane, rows_all).reshape(surface.shape)

    section_one = level_set + time_step * advance(level_set)
    section_two = 0.75 * level_set + 0.25 * (section_one + time_step * advance(section_one))
    advanced = (1.0 / 3.0) * level_set + (2.0 / 3.0) * (section_two + time_step * advance(section_two))
    return advanced - level_set
```

```python
import functools
import math

import jax
import jax.numpy as jnp
import numpy as np
from jax import lax
from jax.experimental import pallas as pl
from jax.experimental.pallas import tpu as pltpu
from jax.sharding import PartitionSpec as P

CELL_SIZE = 0.05
SPEED_LOW = 0.1
SPEED_SPAN = 0.4
TURN_MAX = 1.0
ACCEL_MAX = 0.05
CFL_NUMBER = 0.5
WENO_EPS = 1e-06

LEAN = 1.375
LEVEL = 0.625
REST = 0.609375
UP = 24


def floor_of(spacing):
    return 0.75 * WENO_EPS * spacing * spacing


def squared(value):
    return value * value


def inverse_square(value):
    return squared(1.0 / value)


def one_sided(flow, below_two, below, center, above, above_two, rise, floor):
    ahead = flow > 0.0
    far = jnp.where(ahead, above_two, below_two)
    near = jnp.where(ahead, above, below)
    back = jnp.where(ahead, below, above)
    near_rest = squared(near) * REST + floor
    center_rest = squared(center) * REST + floor
    lean = center * LEAN
    weight_one = inverse_square(squared(far - near * LEAN) + near_rest)
    weight_two = inverse_square(squared(near - center * LEVEL) + center_rest) * 6.0
    weight_three = inverse_square(squared(back - lean) + center_rest) * 3.0
    step = near - center
    fourth_here = (step - (center - back)) * (1.0 / 6.0)
    fourth_near = ((far - near) - step) * (1.0 / 3.0)
    total = weight_one + weight_two + weight_three
    shift = (weight_one * fourth_near + weight_three * fourth_here) / total - 0.5 * fourth_here
    middle = rise - 0.5 * center - (above - below) * (1.0 / 12.0)
    return flow * middle + jnp.abs(flow) * shift


def column_parts(line, floor):
    rise = [line[i + 1] - line[i] for i in range(len(line) - 1)]
    bend = [rise[i + 1] - rise[i] for i in range(len(rise) - 1)]
    turn = [bend[i + 1] - bend[i] for i in range(len(bend) - 1)]
    fourth = [(turn[i + 1] - turn[i]) * (1.0 / 3.0) for i in range(len(turn) - 1)]
    count = len(line) - 6
    at = lambda j: bend[j + 2]
    rest = {j: squared(at(j)) * REST + floor for j in range(-1, count + 1)}
    lean = {j: at(j) * LEAN for j in range(-1, count + 1)}
    to_up = {j: inverse_square(squared(at(j + 1) - lean[j]) + rest[j]) for j in range(0, count + 1)}
    to_down = {j: inverse_square(squared(at(j - 1) - lean[j]) + rest[j]) for j in range(-1, count)}
    pair = {
        j: inverse_square(squared(at(j - 1) - at(j) * LEVEL) + rest[j]) * 6.0
        for j in range(0, count + 1)
    }
    middle = [
        rise[i + 3] - 0.5 * at(i) - (at(i + 1) - at(i - 1)) * (1.0 / 12.0) for i in range(count)
    ]
    return (lambda j: fourth[j + 1]), to_up, to_down, pair, middle


def two_sided(fourth, to_up, to_down, to_up_3, to_down_3, pair, middle, i):
    half = 0.5 * fourth(i)
    right = (to_up[i + 1] * fourth(i + 1) + to_down_3[i] * half) / (
        to_up[i + 1] + to_down_3[i] + pair[i + 1]
    )
    left = (to_down[i - 1] * fourth(i - 1) + to_up_3[i] * half) / (
        to_down[i - 1] + to_up_3[i] + pair[i]
    )
    return jnp.maximum(right + middle[i], left - middle[i]) - 0.5 * half


def picked(flow, fourth, to_up, to_down, pair, middle, i):
    ahead = flow > 0.0
    weight_one = jnp.where(ahead, to_up[i + 1], to_down[i - 1])
    weight_two = jnp.where(ahead, pair[i + 1], pair[i])
    weight_three = jnp.where(ahead, to_down[i], to_up[i]) * 3.0
    far = jnp.where(ahead, fourth(i + 1), fourth(i - 1))
    half = 0.5 * fourth(i)
    shift = (weight_one * far + weight_three * half) / (
        weight_one + weight_two + weight_three
    ) - 0.5 * half
    return flow * middle[i] + jnp.abs(flow) * shift


def speed_kernel(u_ref, out_ref, *, d_speed):
    nx, nh, ny, nv = u_ref.shape
    floor = floor_of(d_speed)
    lane = lax.broadcasted_iota(jnp.int32, (ny, nv), 1)
    first = lane == 0
    last = lane == nv - 1
    inside = jnp.logical_not(jnp.logical_or(first, last))

    def before(value):
        return pltpu.roll(value, 1, 1)

    def after(value):
        return pltpu.roll(value, nv - 1, 1)

    top = 1.0 / (floor * floor)

    def step(k, carry):
        x = k // nh
        h = k % nh
        u = u_ref[x, h]
        rise_here = u - before(u)
        rise_next = after(u) - u
        bend = jnp.where(inside, rise_next - rise_here, 0.0)
        rise = jnp.where(last, rise_here, rise_next)
        below = before(bend)
        above = after(bend)
        rest = squared(bend) * REST + floor
        lean = bend * LEAN
        to_up = inverse_square(squared(above - lean) + rest)
        to_down = inverse_square(squared(below - lean) + rest)
        pair = inverse_square(squared(below - bend * LEVEL) + rest) * 6.0
        fourth = ((above - bend) - (bend - below)) * (1.0 / 3.0)
        half = 0.5 * fourth
        down_before = jnp.where(first, top, before(to_down))
        up_after = jnp.where(last, top, after(to_up))
        fourth_before = jnp.where(first, 0.0, before(fourth))
        fourth_after = jnp.where(last, 0.0, after(fourth))
        up_3 = to_up * 3.0
        down_3 = to_down * 3.0
        middle = rise - 0.5 * bend - (above - below) * (1.0 / 12.0)
        right = (up_after * fourth_after + down_3 * half) / (up_after + down_3 + after(pair))
        left = (down_before * fourth_before + up_3 * half) / (down_before + up_3 + pair)
        out_ref[x, h] = (jnp.maximum(right + middle, left - middle) - 0.5 * half) * (
            ACCEL_MAX / d_speed
        )
        return carry

    lax.fori_loop(0, nx * nh, step, 0, unroll=2)


def ghosts(edge, inner):
    slope = edge - inner
    one = edge + slope
    two = edge + 2.0 * slope
    three = edge + 3.0 * slope
    return one, two, three


def main_kernel(
    flag_ref, dt_ref, u_ref, part_ref, *refs, stage, d_theta
):
    refs = list(refs)
    base_ref = refs.pop(0) if stage > 1 else None
    xlo, xhi, ylo, yhi, hlo, hhi, vel_ref, wind_ref = refs[:8]
    out_ref = refs[8]
    faces = refs[9:-3]
    pad_ref, bend_ref, acc_ref = refs[-3:]
    nx, nh, ny, nv = u_ref.shape
    halves = ny // 8
    floor = floor_of(CELL_SIZE)
    start_x = flag_ref[0] == 1
    end_x = flag_ref[1] == 1
    start_y = flag_ref[2] == 1
    end_y = flag_ref[3] == 1

    def fill(k, carry):
        x = k // nh
        h = k % nh
        pad_ref[k, 8 : 8 + ny] = u_ref[x, h]
        one, two, three = ghosts(u_ref[x, h, 0:1], u_ref[x, h, 1:2])
        low = jnp.concatenate([three, two, one], axis=0)
        pad_ref[k, 5:8] = jnp.where(start_y, low, ylo[x, h])
        one, two, three = ghosts(u_ref[x, h, ny - 1 : ny], u_ref[x, h, ny - 2 : ny - 1])
        high = jnp.concatenate([one, two, three], axis=0)
        pad_ref[k, 8 + ny : 11 + ny] = jnp.where(end_y, high, yhi[x, h])
        return carry

    lax.fori_loop(0, nx * nh, fill, 0, unroll=2)

    def bend(k, carry):
        for r in range(0, UP, 8):
            here = pad_ref[k, r + 6 : r + 14]
            bend_ref[k, r : r + 8] = (pad_ref[k, r + 7 : r + 15] - here) - (
                here - pad_ref[k, r + 5 : r + 13]
            )
        return carry

    lax.fori_loop(0, nx * nh, bend, 0, unroll=2)

    def along_y(k, carry):
        x = k // nh
        h = k % nh
        for half in range(halves):
            r = 8 * half
            flow = vel_ref[1, h] + wind_ref[1, x, r : r + 8]
            rise = pad_ref[k, 9 + r : 17 + r] - pad_ref[k, 8 + r : 16 + r]
            near = [bend_ref[k, r + s : r + s + 8] for s in range(5)]
            acc_ref[x, h, r : r + 8] = part_ref[x, h, r : r + 8] + one_sided(
                flow, *near, rise, floor
            )
        return carry

    lax.fori_loop(0, nx * nh, along_y, 0, unroll=2)

    def along_x(k, carry):
        h = k // halves
        rows = pl.ds(pl.multiple_of((k % halves) * 8, 8), 8)
        mine = [u_ref[x, h, rows] for x in range(nx)]
        low = ghosts(mine[0], mine[1])
        high = ghosts(mine[nx - 1], mine[nx - 2])
        line = (
            [jnp.where(start_x, low[2 - r], xlo[r, h, rows]) for r in range(3)]
            + mine
            + [jnp.where(end_x, high[r], xhi[r, h, rows]) for r in range(3)]
        )
        fourth, to_up, to_down, pair, middle = column_parts(line, floor)
        speed = vel_ref[0, h]
        for x in range(nx):
            flow = speed + wind_ref[0, x, rows]
            acc_ref[x, h, rows] = acc_ref[x, h, rows] + picked(
                flow, fourth, to_up, to_down, pair, middle, x
            )
        return carry

    lax.fori_loop(0, nh * halves, along_x, 0)

    dt = dt_ref[0]
    theta_floor = floor_of(d_theta)

    def along_heading(k, carry):
        x = k // halves
        rows = pl.ds(pl.multiple_of((k % halves) * 8, 8), 8)
        line = (
            [hlo[x, r, rows] for r in range(3)]
            + [u_ref[x, h, rows] for h in range(nh)]
            + [hhi[x, r, rows] for r in range(3)]
        )
        fourth, to_up, to_down, pair, middle = column_parts(line, theta_floor)
        up_3 = {j: to_up[j] * 3.0 for j in range(nh)}
        down_3 = {j: to_down[j] * 3.0 for j in range(nh)}
        for h in range(nh):
            term = two_sided(fourth, to_up, to_down, up_3, down_3, pair, middle, h)
            change = dt * jnp.minimum(acc_ref[x, h, rows] + term * (TURN_MAX / d_theta), 0.0)
            u = line[h + 3]
            if stage == 1:
                value = u + change
            elif stage == 2:
                value = 0.75 * base_ref[x, h, rows] + 0.25 * (u + change)
            else:
                value = (2.0 / 3.0) * ((u - base_ref[x, h, rows]) + change)
            out_ref[x, h, rows] = value
            if stage < 3:
                if h < 3:
                    faces[2][x, h, rows] = value
                if h >= nh - 3:
                    faces[3][x, h - nh + 3, rows] = value
        return carry

    lax.fori_loop(0, nx * halves, along_heading, 0)

    if stage < 3:

        def edge(k, carry):
            x = k // nh
            h = k % nh
            faces[0][x, h] = out_ref[x, h, 0:3]
            faces[1][x, h] = out_ref[x, h, ny - 3 : ny]
            return carry

        lax.fori_loop(0, nx * nh, edge, 0, unroll=4)


def rate_kernel(table_ref, wind_ref, out_ref):
    fast_x = jnp.abs(table_ref[0] + wind_ref[0])
    fast_y = jnp.abs(table_ref[1] + wind_ref[1])
    out_ref[0, 0] = jnp.max(fast_x + fast_y)


VMEM = pl.BlockSpec(memory_space=pltpu.VMEM)
SMEM = pl.BlockSpec(memory_space=pltpu.SMEM)


def ring(count, step):
    return [(i, (i + step) % count) for i in range(count)]


def body(level_set, wind_field):
    field = jnp.transpose(level_set, (0, 2, 1, 3))
    nx, nh, ny, nv = field.shape
    n_head = nh * lax.axis_size("ha")
    d_theta = 2.0 * math.pi / n_head
    d_speed = SPEED_SPAN / nv
    gx, gy = lax.axis_index("gx"), lax.axis_index("gy")
    flags = jnp.stack(
        [gx == 0, gx == lax.axis_size("gx") - 1, gy == 0, gy == lax.axis_size("gy") - 1]
    ).astype(jnp.int32)

    every_angle = np.arange(n_head, dtype=np.float32) * np.float32(d_theta)
    ends = [SPEED_LOW + SPEED_SPAN * 0.5 / nv, SPEED_LOW + SPEED_SPAN * (nv - 0.5) / nv]
    table = np.stack(
        [
            np.concatenate([np.float32(v) * way(every_angle) for v in ends])
            for way in (np.cos, np.sin)
        ]
    ).astype(np.float32)
    table = np.ascontiguousarray(np.broadcast_to(table[:, :, None], (*table.shape, nx * ny)))
    local_top = pl.pallas_call(
        rate_kernel,
        out_shape=jax.ShapeDtypeStruct((1, 1), jnp.float32),
        in_specs=[VMEM, VMEM],
        out_specs=SMEM,
        name="rate",
    )(jnp.asarray(table), wind_field.reshape(2, 1, nx * ny))[0, 0]

    speeds = SPEED_LOW + SPEED_SPAN * (jnp.arange(nv, dtype=jnp.float32) + 0.5) / nv
    angles = (lax.axis_index("ha") * nh + jnp.arange(nh, dtype=jnp.int32)).astype(
        jnp.float32
    ) * d_theta
    heading = jnp.stack([jnp.cos(angles), jnp.sin(angles)])
    velocity = heading[:, :, None, None] * jnp.broadcast_to(
        speeds * (1.0 / CELL_SIZE), (2, nh, 8, nv)
    )
    wind = jnp.broadcast_to((wind_field * (1.0 / CELL_SIZE))[..., None], (2, nx, ny, nv))

    shape = jax.ShapeDtypeStruct(field.shape, jnp.float32)
    x_face = jax.ShapeDtypeStruct((3, nh, ny, nv), jnp.float32)
    y_face = jax.ShapeDtypeStruct((nx, nh, 3, nv), jnp.float32)
    h_face = jax.ShapeDtypeStruct((nx, 3, ny, nv), jnp.float32)

    def speed_part(u):
        return pl.pallas_call(
            functools.partial(speed_kernel, d_speed=d_speed),
            out_shape=shape,
            in_specs=[VMEM],
            out_specs=VMEM,
            cost_estimate=pl.CostEstimate(
                flops=100 * nx * nh * ny * nv, bytes_accessed=8 * nx * nh * ny * nv, transcendentals=0
            ),
            compiler_params=pltpu.CompilerParams(vmem_limit_bytes=8 << 20),
            name="speed",
        )(u)

    def main(stage, u, part, halos, time_step, base):
        outs = [shape]
        if stage < 3:
            outs += [y_face, y_face, h_face, h_face]
        ins = [flags, time_step, u, part] + ([base] if stage > 1 else []) + [*halos, velocity, wind]
        return pl.pallas_call(
            functools.partial(main_kernel, stage=stage, d_theta=d_theta),
            out_shape=outs,
            in_specs=[SMEM, SMEM] + [VMEM] * (len(ins) - 2),
            out_specs=[VMEM] * len(outs),
            scratch_shapes=[
                pltpu.VMEM((nx * nh, ny + 16, nv), jnp.float32),
                pltpu.VMEM((nx * nh, UP, nv), jnp.float32),
                pltpu.VMEM((nx, nh, ny, nv), jnp.float32),
            ],
            cost_estimate=pl.CostEstimate(
                flops=300 * nx * nh * ny * nv, bytes_accessed=16 * nx * nh * ny * nv, transcendentals=0
            ),
            compiler_params=pltpu.CompilerParams(vmem_limit_bytes=24 << 20),
            name=f"main{stage}",
        )(*ins)

    def exchange(u, y_first, y_last, h_first, h_last):
        xlo = lax.ppermute(u[nx - 3 :], "gx", ring(lax.axis_size("gx"), 1))
        xhi = lax.ppermute(u[:3], "gx", ring(lax.axis_size("gx"), -1))
        hlo = lax.ppermute(h_last, "ha", ring(lax.axis_size("ha"), 1))
        hhi = lax.ppermute(h_first, "ha", ring(lax.axis_size("ha"), -1))
        ylo = lax.ppermute(y_last, "gy", ring(lax.axis_size("gy"), 1))
        yhi = lax.ppermute(y_first, "gy", ring(lax.axis_size("gy"), -1))
        return xlo, xhi, ylo, yhi, hlo, hhi

    faces = (field[:, :, :3], field[:, :, ny - 3 :], field[:, :3], field[:, nh - 3 :])
    halos = exchange(field, *faces)
    copies = jnp.broadcast_to(local_top, (lax.axis_size(("gx", "gy")), 1, 1))
    tops = lax.all_to_all(copies, ("gx", "gy"), split_axis=0, concat_axis=0, tiled=True)
    top_rate = jnp.max(tops) / CELL_SIZE + TURN_MAX / d_theta + ACCEL_MAX / d_speed
    time_step = (CFL_NUMBER / top_rate).reshape(1)

    u = field
    for stage in (1, 2, 3):
        part = speed_part(u)
        u, *faces = main(stage, u, part, halos, time_step, field)
        if stage < 3:
            halos = exchange(u, *faces)
    return jnp.transpose(u, (0, 2, 1, 3))


def solution(mesh):
    return jax.shard_map(
        body,
        mesh=mesh,
        in_specs=(P("gx", "gy", "ha", None), P(None, "gx", "gy")),
        out_specs=P("gx", "gy", "ha", None),
        check_vma=False,
    )
```

```python
import functools
import math

import jax
import jax.numpy as jnp
import numpy as np
from jax import lax
from jax.experimental import pallas as pl
from jax.experimental.pallas import tpu as pltpu
from jax.sharding import PartitionSpec as P


CELL_SIZE = 0.05
SPEED_LOW = 0.1
SPEED_SPAN = 0.4
TURN_MAX = 1.0
ACCEL_MAX = 0.05
CFL_NUMBER = 0.5
WENO_EPS = 1e-06

LEAN = 1.375
LEVEL = 0.625
REST = 0.609375
UP = 24


def floor_of(spacing):
    return 0.75 * WENO_EPS * spacing * spacing


def squared(value):
    return value * value


def inverse_square(value):
    return squared(1.0 / value)


def one_sided(flow, below_two, below, center, above, above_two, across, floor):
    ahead = flow > 0.0
    far = jnp.where(ahead, above_two, below_two)
    near = jnp.where(ahead, above, below)
    back = jnp.where(ahead, below, above)
    near_rest = squared(near) * REST + floor
    center_rest = squared(center) * REST + floor
    weight_one = inverse_square(squared(far - near * LEAN) + near_rest)
    weight_two = inverse_square(squared(near - center * LEVEL) + center_rest) * 6.0
    weight_three = inverse_square(squared(back - center * LEAN) + center_rest) * 3.0
    step = near - center
    fourth_here = (step - (center - back)) * (1.0 / 3.0)
    fourth_near = ((far - near) - step) * (2.0 / 3.0)
    total = weight_one + weight_two + weight_three
    shift = (weight_one * fourth_near + weight_three * fourth_here) / total - 0.5 * fourth_here
    middle = across - (above - below) * (1.0 / 6.0)
    return flow * middle + jnp.abs(flow) * shift


def column_parts(line, floor):
    rise = [line[i + 1] - line[i] for i in range(len(line) - 1)]
    bend = [rise[i + 1] - rise[i] for i in range(len(rise) - 1)]
    turn = [bend[i + 1] - bend[i] for i in range(len(bend) - 1)]
    fourth = [(turn[i + 1] - turn[i]) * (2.0 / 3.0) for i in range(len(turn) - 1)]
    count = len(line) - 6
    at = lambda j: bend[j + 2]
    rest = {j: squared(at(j)) * REST + floor for j in range(-1, count + 1)}
    lean = {j: at(j) * LEAN for j in range(-1, count + 1)}
    to_up = {j: inverse_square(squared(at(j + 1) - lean[j]) + rest[j]) for j in range(0, count + 1)}
    to_down = {j: inverse_square(squared(at(j - 1) - lean[j]) + rest[j]) for j in range(-1, count)}
    pair = {
        j: inverse_square(squared(at(j - 1) - at(j) * LEVEL) + rest[j]) * 6.0
        for j in range(0, count + 1)
    }
    middle = [
        (line[i + 4] - line[i + 2]) - (at(i + 1) - at(i - 1)) * (1.0 / 6.0) for i in range(count)
    ]
    return (lambda j: fourth[j + 1]), to_up, to_down, pair, middle


def two_sided(fourth, to_up, to_down, to_up_3, to_down_3, pair, middle, i):
    half = 0.5 * fourth(i)
    right = (to_up[i + 1] * fourth(i + 1) + to_down_3[i] * half) / (
        to_up[i + 1] + to_down_3[i] + pair[i + 1]
    )
    left = (to_down[i - 1] * fourth(i - 1) + to_up_3[i] * half) / (
        to_down[i - 1] + to_up_3[i] + pair[i]
    )
    return jnp.maximum(right + middle[i], left - middle[i]) - 0.5 * half


def picked(flow, fourth, to_up, to_down, pair, middle, i):
    ahead = flow > 0.0
    weight_one = jnp.where(ahead, to_up[i + 1], to_down[i - 1])
    weight_two = jnp.where(ahead, pair[i + 1], pair[i])
    weight_three = jnp.where(ahead, to_down[i], to_up[i]) * 3.0
    far = jnp.where(ahead, fourth(i + 1), fourth(i - 1))
    half = 0.5 * fourth(i)
    shift = (weight_one * far + weight_three * half) / (
        weight_one + weight_two + weight_three
    ) - 0.5 * half
    return flow * middle[i] + jnp.abs(flow) * shift


def speed_kernel(u_ref, out_ref, *, d_speed):
    nx, nh, ny, nv = u_ref.shape
    floor = floor_of(d_speed)
    lane = lax.broadcasted_iota(jnp.int32, (ny, nv), 1)
    first = lane == 0
    last = lane == nv - 1
    inside = jnp.logical_not(jnp.logical_or(first, last))

    def before(value):
        return pltpu.roll(value, 1, 1)

    def after(value):
        return pltpu.roll(value, nv - 1, 1)

    top = 1.0 / (floor * floor)

    def one(x, h):
        u = u_ref[x, h]
        u_before = before(u)
        u_after = after(u)
        rise_here = u - u_before
        rise_next = u_after - u
        bend = jnp.where(inside, rise_next - rise_here, 0.0)
        across = jnp.where(
            first, 2.0 * rise_next, jnp.where(last, 2.0 * rise_here, u_after - u_before)
        )
        below = before(bend)
        above = after(bend)
        rest = squared(bend) * REST + floor
        lean = bend * LEAN
        to_up = inverse_square(squared(above - lean) + rest)
        to_down = inverse_square(squared(below - lean) + rest)
        pair = inverse_square(squared(below - bend * LEVEL) + rest) * 6.0
        fourth = ((above - bend) - (bend - below)) * (2.0 / 3.0)
        half = 0.5 * fourth
        down_before = jnp.where(first, top, before(to_down))
        up_after = jnp.where(last, top, after(to_up))
        fourth_before = jnp.where(first, 0.0, before(fourth))
        fourth_after = jnp.where(last, 0.0, after(fourth))
        up_3 = to_up * 3.0
        down_3 = to_down * 3.0
        middle = across - (above - below) * (1.0 / 6.0)
        right = (up_after * fourth_after + down_3 * half) / (up_after + down_3 + after(pair))
        left = (down_before * fourth_before + up_3 * half) / (down_before + up_3 + pair)
        out_ref[x, h] = (jnp.maximum(right + middle, left - middle) - 0.5 * half) * (
            0.5 * ACCEL_MAX / d_speed
        )

    def step(x, carry):
        for h in range(nh):
            one(x, h)
        return carry

    lax.fori_loop(0, nx, step, 0)


def ghosts(edge, inner):
    slope = edge - inner
    one = edge + slope
    two = one + slope
    return one, two, two + slope


def plane_kernel(
    flag_ref, u_ref, part_ref, xlo, xhi, ylo, yhi, vel_ref, wind_ref, acc_ref, pad_ref, bend_ref
):
    nx, nh, ny, nv = u_ref.shape
    halves = ny // 8
    floor = floor_of(CELL_SIZE)
    start_x = flag_ref[0] == 1
    end_x = flag_ref[1] == 1
    start_y = flag_ref[2] == 1
    end_y = flag_ref[3] == 1
    row = lax.broadcasted_iota(jnp.int32, (3, nv), 0).astype(jnp.float32)
    reach_low = 3.0 - row
    reach_high = 1.0 + row

    def fill(x, carry):
        for h in range(nh):
            pad_ref[x, h, 8 : 8 + ny] = u_ref[x, h]
            edge = u_ref[x, h, pl.ds(0, 3, stride=0)]
            inner = u_ref[x, h, pl.ds(1, 3, stride=0)]
            pad_ref[x, h, 5:8] = jnp.where(start_y, edge + reach_low * (edge - inner), ylo[x, h])
            edge = u_ref[x, h, pl.ds(ny - 1, 3, stride=0)]
            inner = u_ref[x, h, pl.ds(ny - 2, 3, stride=0)]
            pad_ref[x, h, 8 + ny : 11 + ny] = jnp.where(
                end_y, edge + reach_high * (edge - inner), yhi[x, h]
            )
        for h in range(nh):
            for r in range(0, UP, 8):
                here = pad_ref[x, h, r + 6 : r + 14]
                bend_ref[x, h, r : r + 8] = (pad_ref[x, h, r + 7 : r + 15] - here) - (
                    here - pad_ref[x, h, r + 5 : r + 13]
                )
        return carry

    lax.fori_loop(0, nx, fill, 0)

    def along_y(x, carry):
        for h in range(nh):
            for r in range(0, ny, 8):
                flow = vel_ref[1, h] + wind_ref[1, x, r : r + 8]
                across = pad_ref[x, h, 9 + r : 17 + r] - pad_ref[x, h, 7 + r : 15 + r]
                near = [bend_ref[x, h, r + s : r + s + 8] for s in range(5)]
                acc_ref[x, h, r : r + 8] = part_ref[x, h, r : r + 8] + one_sided(
                    flow, *near, across, floor
                )
        return carry

    lax.fori_loop(0, nx, along_y, 0)

    def along_x(h, carry):
        for half in range(halves):
            rows = slice(8 * half, 8 * half + 8)
            mine = [u_ref[x, h, rows] for x in range(nx)]
            low = ghosts(mine[0], mine[1])
            high = ghosts(mine[nx - 1], mine[nx - 2])
            line = (
                [jnp.where(start_x, low[2 - r], xlo[r, h, rows]) for r in range(3)]
                + mine
                + [jnp.where(end_x, high[r], xhi[r, h, rows]) for r in range(3)]
            )
            fourth, to_up, to_down, pair, middle = column_parts(line, floor)
            speed = vel_ref[0, h]
            for x in range(nx):
                flow = speed + wind_ref[0, x, rows]
                acc_ref[x, h, rows] = acc_ref[x, h, rows] + picked(
                    flow, fourth, to_up, to_down, pair, middle, x
                )
        return carry

    lax.fori_loop(0, nh, along_x, 0)


def heading_kernel(dt_ref, u_ref, acc_ref, *refs, stage, d_theta):
    refs = list(refs)
    base_ref = refs.pop(0) if stage > 1 else None
    hlo, hhi, out_ref, *faces = refs
    nx, nh, ny, _ = u_ref.shape
    halves = ny // 8
    dt = dt_ref[0]
    theta_floor = floor_of(d_theta)

    def along_heading(x, carry):
        for half in range(halves):
            rows = slice(8 * half, 8 * half + 8)
            line = (
                [hlo[x, r, rows] for r in range(3)]
                + [u_ref[x, h, rows] for h in range(nh)]
                + [hhi[x, r, rows] for r in range(3)]
            )
            fourth, to_up, to_down, pair, middle = column_parts(line, theta_floor)
            up_3 = {j: to_up[j] * 3.0 for j in range(nh)}
            down_3 = {j: to_down[j] * 3.0 for j in range(nh)}
            for h in range(nh):
                term = two_sided(fourth, to_up, to_down, up_3, down_3, pair, middle, h)
                change = dt * jnp.minimum(
                    acc_ref[x, h, rows] + term * (0.5 * TURN_MAX / d_theta), 0.0
                )
                u = line[h + 3]
                if stage == 1:
                    value = u + change
                elif stage == 2:
                    value = 0.75 * base_ref[x, h, rows] + 0.25 * (u + change)
                else:
                    value = (2.0 / 3.0) * ((u - base_ref[x, h, rows]) + change)
                out_ref[x, h, rows] = value
                if stage < 3:
                    if h < 3:
                        faces[2][x, h, rows] = value
                    if h >= nh - 3:
                        faces[3][x, h - nh + 3, rows] = value
                    if half == 0:
                        faces[0][x, h] = value[0:3]
        if stage < 3:
            for h in range(nh):
                faces[1][x, h] = out_ref[x, h, ny - 3 : ny]
        return carry

    lax.fori_loop(0, nx, along_heading, 0)


def rate_kernel(wind_ref, out_ref, *, spots):
    wind_x = wind_ref[0]
    wind_y = wind_ref[1]
    top = None
    for move_x, move_y in spots:
        fast = jnp.abs(wind_x + move_x) + jnp.abs(wind_y + move_y)
        top = fast if top is None else jnp.maximum(top, fast)
    out_ref[...] = jnp.full(out_ref.shape, jnp.max(top), jnp.float32)


VMEM = pl.BlockSpec(memory_space=pltpu.VMEM)
SMEM = pl.BlockSpec(memory_space=pltpu.SMEM)


def ring(count, step):
    return [(i, (i + step) % count) for i in range(count)]


def body(level_set, wind_field):
    field = jnp.transpose(level_set, (0, 2, 1, 3))
    nx, nh, ny, nv = field.shape
    n_head = nh * lax.axis_size("ha")
    d_theta = 2.0 * math.pi / n_head
    d_speed = SPEED_SPAN / nv
    gx, gy = lax.axis_index("gx"), lax.axis_index("gy")
    flags = jnp.stack(
        [gx == 0, gx == lax.axis_size("gx") - 1, gy == 0, gy == lax.axis_size("gy") - 1]
    ).astype(jnp.int32)

    every_angle = np.arange(n_head, dtype=np.float32) * np.float32(d_theta)
    ends = [SPEED_LOW + SPEED_SPAN * 0.5 / nv, SPEED_LOW + SPEED_SPAN * (nv - 0.5) / nv]
    spots = [
        (float(np.float32(v) * np.cos(angle)), float(np.float32(v) * np.sin(angle)))
        for v in ends
        for angle in every_angle
    ]
    top = pl.pallas_call(
        functools.partial(rate_kernel, spots=spots),
        out_shape=jax.ShapeDtypeStruct((8, 128), jnp.float32),
        in_specs=[VMEM],
        out_specs=VMEM,
        compiler_params=pltpu.CompilerParams(vmem_limit_bytes=4 << 20),
        name="rate",
    )(wind_field)

    speeds = SPEED_LOW + SPEED_SPAN * (jnp.arange(nv, dtype=jnp.float32) + 0.5) / nv
    angles = (lax.axis_index("ha") * nh + jnp.arange(nh, dtype=jnp.int32)).astype(
        jnp.float32
    ) * d_theta
    heading = jnp.stack([jnp.cos(angles), jnp.sin(angles)])
    velocity = heading[:, :, None, None] * jnp.broadcast_to(
        speeds * (0.5 / CELL_SIZE), (2, nh, 8, nv)
    )
    wind = jnp.broadcast_to((wind_field * (0.5 / CELL_SIZE))[..., None], (2, nx, ny, nv))

    shape = jax.ShapeDtypeStruct(field.shape, jnp.float32)
    y_face = jax.ShapeDtypeStruct((nx, nh, 3, nv), jnp.float32)
    h_face = jax.ShapeDtypeStruct((nx, 3, ny, nv), jnp.float32)

    def speed_part(u):
        return pl.pallas_call(
            functools.partial(speed_kernel, d_speed=d_speed),
            out_shape=shape,
            in_specs=[VMEM],
            out_specs=VMEM,
            cost_estimate=pl.CostEstimate(
                flops=100 * nx * nh * ny * nv, bytes_accessed=8 * nx * nh * ny * nv, transcendentals=0
            ),
            compiler_params=pltpu.CompilerParams(vmem_limit_bytes=8 << 20),
            name="speed",
        )(u)

    def plane_part(u, part, xlo, xhi, ylo, yhi):
        return pl.pallas_call(
            plane_kernel,
            out_shape=shape,
            in_specs=[SMEM] + [VMEM] * 8,
            out_specs=VMEM,
            scratch_shapes=[
                pltpu.VMEM((nx, nh, ny + 16, nv), jnp.float32),
                pltpu.VMEM((nx, nh, UP, nv), jnp.float32),
            ],
            cost_estimate=pl.CostEstimate(
                flops=200 * nx * nh * ny * nv, bytes_accessed=16 * nx * nh * ny * nv, transcendentals=0
            ),
            compiler_params=pltpu.CompilerParams(vmem_limit_bytes=24 << 20),
            name="plane",
        )(flags, u, part, xlo, xhi, ylo, yhi, velocity, wind)

    def heading_part(stage, u, acc, hlo, hhi):
        outs = [shape]
        if stage < 3:
            outs += [y_face, y_face, h_face, h_face]
        ins = [time_step, u, acc] + ([field] if stage > 1 else []) + [hlo, hhi]
        return pl.pallas_call(
            functools.partial(heading_kernel, stage=stage, d_theta=d_theta),
            out_shape=outs,
            in_specs=[SMEM] + [VMEM] * (len(ins) - 1),
            out_specs=[VMEM] * len(outs),
            cost_estimate=pl.CostEstimate(
                flops=100 * nx * nh * ny * nv, bytes_accessed=16 * nx * nh * ny * nv, transcendentals=0
            ),
            compiler_params=pltpu.CompilerParams(vmem_limit_bytes=24 << 20),
        )(*ins)

    def exchange(u, y_first, y_last, h_first, h_last):
        def halo(value, axis, step):
            return lax.ppermute(value, axis, ring(lax.axis_size(axis), step))

        xlo = halo(u[nx - 3 :], "gx", 1)
        xhi = halo(u[:3], "gx", -1)
        ylo = halo(y_last, "gy", 1)
        yhi = halo(y_first, "gy", -1)
        hlo = halo(h_last, "ha", 1)
        hhi = halo(h_first, "ha", -1)
        return xlo, xhi, ylo, yhi, hlo, hhi

    for axis, bit in [("gx", 1), ("gx", 2), ("gy", 1), ("gy", 2), ("gy", 4)]:
        other = lax.ppermute(top, axis, [(j, j ^ bit) for j in range(lax.axis_size(axis))])
        top = jnp.maximum(top, other)
    top_rate = top[0, :1] / CELL_SIZE + TURN_MAX / d_theta + ACCEL_MAX / d_speed
    time_step = CFL_NUMBER / top_rate

    u = field
    faces = (field[:, :, :3], field[:, :, ny - 3 :], field[:, :3], field[:, nh - 3 :])
    for stage in (1, 2, 3):
        xlo, xhi, ylo, yhi, hlo, hhi = exchange(u, *faces)
        part = speed_part(u)
        acc = plane_part(u, part, xlo, xhi, ylo, yhi)
        u, *faces = heading_part(stage, u, acc, hlo, hhi)
    return jnp.transpose(u, (0, 2, 1, 3))


def solution(mesh):
    return jax.shard_map(
        body,
        mesh=mesh,
        in_specs=(P("gx", "gy", "ha", None), P(None, "gx", "gy")),
        out_specs=P("gx", "gy", "ha", None),
        check_vma=False,
    )
```

```python
import functools
import math

import jax
import jax.numpy as jnp
import numpy as np
from jax import lax
from jax.experimental import pallas as pl
from jax.experimental.pallas import tpu as pltpu
from jax.sharding import PartitionSpec as P


CELL_SIZE = 0.05
SPEED_LOW = 0.1
SPEED_SPAN = 0.4
TURN_MAX = 1.0
ACCEL_MAX = 0.05
CFL_NUMBER = 0.5
WENO_EPS = 1e-06

LEAN = 1.375
LEVEL = 0.625
REST = 0.609375
UP = 24


def floor_of(spacing):
    return 0.75 * WENO_EPS * spacing * spacing


def squared(value):
    return value * value


def inverse_square(value):
    return squared(1.0 / value)


def one_sided(flow, below_two, below, center, above, above_two, across, floor):
    ahead = flow > 0.0
    far = jnp.where(ahead, above_two, below_two)
    near = jnp.where(ahead, above, below)
    back = jnp.where(ahead, below, above)
    near_rest = squared(near) * REST + floor
    center_rest = squared(center) * REST + floor
    weight_one = inverse_square(squared(far - near * LEAN) + near_rest)
    weight_two = inverse_square(squared(near - center * LEVEL) + center_rest) * 6.0
    weight_three = inverse_square(squared(back - center * LEAN) + center_rest) * 3.0
    step = near - center
    fourth_here = (step - (center - back)) * (1.0 / 3.0)
    fourth_near = ((far - near) - step) * (2.0 / 3.0)
    total = weight_one + weight_two + weight_three
    shift = (weight_one * fourth_near + weight_three * fourth_here) / total - 0.5 * fourth_here
    middle = across - (above - below) * (1.0 / 6.0)
    return flow * middle + jnp.abs(flow) * shift


def column_parts(line, floor):
    rise = [line[i + 1] - line[i] for i in range(len(line) - 1)]
    bend = [rise[i + 1] - rise[i] for i in range(len(rise) - 1)]
    turn = [bend[i + 1] - bend[i] for i in range(len(bend) - 1)]
    fourth = [(turn[i + 1] - turn[i]) * (2.0 / 3.0) for i in range(len(turn) - 1)]
    count = len(line) - 6
    at = lambda j: bend[j + 2]
    rest = {j: squared(at(j)) * REST + floor for j in range(-1, count + 1)}
    lean = {j: at(j) * LEAN for j in range(-1, count + 1)}
    to_up = {j: inverse_square(squared(at(j + 1) - lean[j]) + rest[j]) for j in range(0, count + 1)}
    to_down = {j: inverse_square(squared(at(j - 1) - lean[j]) + rest[j]) for j in range(-1, count)}
    pair = {
        j: inverse_square(squared(at(j - 1) - at(j) * LEVEL) + rest[j]) * 6.0
        for j in range(0, count + 1)
    }
    middle = [
        (line[i + 4] - line[i + 2]) - (at(i + 1) - at(i - 1)) * (1.0 / 6.0) for i in range(count)
    ]
    return (lambda j: fourth[j + 1]), to_up, to_down, pair, middle


def two_sided(fourth, to_up, to_down, to_up_3, to_down_3, pair, middle, i):
    half = 0.5 * fourth(i)
    right = (to_up[i + 1] * fourth(i + 1) + to_down_3[i] * half) / (
        to_up[i + 1] + to_down_3[i] + pair[i + 1]
    )
    left = (to_down[i - 1] * fourth(i - 1) + to_up_3[i] * half) / (
        to_down[i - 1] + to_up_3[i] + pair[i]
    )
    return jnp.maximum(right + middle[i], left - middle[i]) - 0.5 * half


def picked(flow, fourth, to_up, to_down, pair, middle, i):
    ahead = flow > 0.0
    weight_one = jnp.where(ahead, to_up[i + 1], to_down[i - 1])
    weight_two = jnp.where(ahead, pair[i + 1], pair[i])
    weight_three = jnp.where(ahead, to_down[i], to_up[i]) * 3.0
    far = jnp.where(ahead, fourth(i + 1), fourth(i - 1))
    half = 0.5 * fourth(i)
    shift = (weight_one * far + weight_three * half) / (
        weight_one + weight_two + weight_three
    ) - 0.5 * half
    return flow * middle[i] + jnp.abs(flow) * shift


def speed_kernel(u_ref, *refs, d_speed, blocks):
    out_ref, turned, bent, up_ref, down_ref, pair_ref, fourth_ref, done_ref = refs[-8:]
    nv = u_ref.shape[1]
    floor = floor_of(d_speed)
    top = 1.0 / (floor * floor)
    first, last = 8, 8 + nv

    for b in range(*blocks):
        turned[b, first:last] = u_ref[128 * b : 128 * b + 128].T

    def bends(b, carry):
        zero = jnp.zeros((8, 128), jnp.float32)
        turned[b, first - 1 : first] = (
            2.0 * turned[b, first : first + 1] - turned[b, first + 1 : first + 2]
        )
        turned[b, last : last + 1] = (
            2.0 * turned[b, last - 1 : last] - turned[b, last - 2 : last - 1]
        )
        for ref, low, high in (
            (bent, zero, zero),
            (fourth_ref, zero, zero),
            (down_ref, zero + top, None),
            (up_ref, None, zero + top),
            (pair_ref, None, zero + 6.0 * top),
        ):
            if low is not None:
                ref[b, first - 8 : first] = low
            if high is not None:
                ref[b, last : last + 8] = high
        for r in range(first, last, 8):
            here = turned[b, r : r + 8]
            bent[b, r : r + 8] = (turned[b, r + 1 : r + 9] - here) - (
                here - turned[b, r - 1 : r + 7]
            )
        return carry

    lax.fori_loop(*blocks, bends, 0)

    def weights(b, carry):
        for r in range(first, last, 8):
            below, bend, above = (bent[b, r + d : r + d + 8] for d in (-1, 0, 1))
            rest = squared(bend) * REST + floor
            lean = bend * LEAN
            up_ref[b, r : r + 8] = inverse_square(squared(above - lean) + rest)
            down_ref[b, r : r + 8] = inverse_square(squared(below - lean) + rest)
            pair_ref[b, r : r + 8] = inverse_square(squared(below - bend * LEVEL) + rest) * 6.0
            fourth_ref[b, r : r + 8] = ((above - bend) - (bend - below)) * (2.0 / 3.0)
        return carry

    lax.fori_loop(*blocks, weights, 0)

    def combine(b, carry):
        for r in range(first, last, 8):
            half = 0.5 * fourth_ref[b, r : r + 8]
            up_3 = up_ref[b, r : r + 8] * 3.0
            down_3 = down_ref[b, r : r + 8] * 3.0
            up_after = up_ref[b, r + 1 : r + 9]
            down_before = down_ref[b, r - 1 : r + 7]
            middle = (turned[b, r + 1 : r + 9] - turned[b, r - 1 : r + 7]) - (
                bent[b, r + 1 : r + 9] - bent[b, r - 1 : r + 7]
            ) * (1.0 / 6.0)
            right = (up_after * fourth_ref[b, r + 1 : r + 9] + down_3 * half) / (
                up_after + down_3 + pair_ref[b, r + 1 : r + 9]
            )
            left = (down_before * fourth_ref[b, r - 1 : r + 7] + up_3 * half) / (
                down_before + up_3 + pair_ref[b, r : r + 8]
            )
            done_ref[b, r : r + 8] = (jnp.maximum(right + middle, left - middle) - 0.5 * half) * (
                0.5 * ACCEL_MAX / d_speed
            )
        return carry

    lax.fori_loop(*blocks, combine, 0)
    for b in range(*blocks):
        out_ref[128 * b : 128 * b + 128] = done_ref[b, first:last].T


def ghosts(edge, inner):
    slope = edge - inner
    one = edge + slope
    two = one + slope
    return one, two, two + slope


def plane_kernel(
    u_ref, part_ref, xlo, xhi, ymate, yother, vel_ref, wind_ref, acc_ref, pad_ref, bend_ref
):
    nx, nh, ny, nv = u_ref.shape
    halves = ny // 8
    floor = floor_of(CELL_SIZE)
    gx, gy = lax.axis_index("gx"), lax.axis_index("gy")
    start_x = gx == 0
    end_x = gx == lax.axis_size("gx") - 1
    at_edge = jnp.logical_or(gy == 0, gy == lax.axis_size("gy") - 1)
    odd = lax.rem(gy, 2)
    mate_at = 8 + ny - odd * (ny + 3)
    other_at = 5 + odd * (ny + 3)
    edge_row = odd * (ny - 1)
    inner_row = 1 + odd * (ny - 3)
    row = lax.broadcasted_iota(jnp.int32, (3, nv), 0)
    reach = (3 - row + odd * (2 * row - 2)).astype(jnp.float32)

    def fill(x, carry):
        for h in range(nh):
            pad_ref[x, h, 8 : 8 + ny] = u_ref[x, h]
            pad_ref[x, h, pl.ds(mate_at, 3)] = ymate[x, h]
            edge = u_ref[x, h, pl.ds(edge_row, 3, stride=0)]
            inner = u_ref[x, h, pl.ds(inner_row, 3, stride=0)]
            pad_ref[x, h, pl.ds(other_at, 3)] = jnp.where(
                at_edge, edge + reach * (edge - inner), yother[x, h]
            )
        for h in range(nh):
            for r in range(0, UP, 8):
                here = pad_ref[x, h, r + 6 : r + 14]
                bend_ref[x, h, r : r + 8] = (pad_ref[x, h, r + 7 : r + 15] - here) - (
                    here - pad_ref[x, h, r + 5 : r + 13]
                )
        return carry

    lax.fori_loop(0, nx, fill, 0)

    def along_y(x, carry):
        for h in range(nh):
            for r in range(0, ny, 8):
                flow = vel_ref[1, h] + wind_ref[1, x, r : r + 8]
                across = pad_ref[x, h, 9 + r : 17 + r] - pad_ref[x, h, 7 + r : 15 + r]
                near = [bend_ref[x, h, r + s : r + s + 8] for s in range(5)]
                acc_ref[x, h, r : r + 8] = part_ref[x, h, r : r + 8] + one_sided(
                    flow, *near, across, floor
                )
        return carry

    lax.fori_loop(0, nx, along_y, 0)

    def along_x(h, carry):
        for half in range(halves):
            rows = slice(8 * half, 8 * half + 8)
            mine = [u_ref[x, h, rows] for x in range(nx)]
            low = ghosts(mine[0], mine[1])
            high = ghosts(mine[nx - 1], mine[nx - 2])
            line = (
                [jnp.where(start_x, low[2 - r], xlo[r, h, rows]) for r in range(3)]
                + mine
                + [jnp.where(end_x, high[r], xhi[r, h, rows]) for r in range(3)]
            )
            fourth, to_up, to_down, pair, middle = column_parts(line, floor)
            speed = vel_ref[0, h]
            for x in range(nx):
                flow = speed + wind_ref[0, x, rows]
                acc_ref[x, h, rows] = acc_ref[x, h, rows] + picked(
                    flow, fourth, to_up, to_down, pair, middle, x
                )
        return carry

    lax.fori_loop(0, nh, along_x, 0)


def heading_kernel(top_ref, u_ref, acc_ref, *refs, stage, d_theta, d_speed):
    refs = list(refs)
    base_ref = refs.pop(0) if stage > 1 else None
    hlo, hhi, out_ref, *faces = refs
    if stage == 3:
        whole_ref, out_ref, sent = out_ref, *faces
        faces = None
    nx, nh, ny, _ = u_ref.shape
    halves = ny // 8
    mate_row = (1 - lax.rem(lax.axis_index("gy"), 2)) * (ny - 3)
    dt = CFL_NUMBER / (
        top_ref[...] * (1.0 / CELL_SIZE) + (TURN_MAX / d_theta + ACCEL_MAX / d_speed)
    )
    theta_floor = floor_of(d_theta)

    def along_heading(x, carry):
        for half in range(halves):
            rows = slice(8 * half, 8 * half + 8)
            line = (
                [hlo[x, r, rows] for r in range(3)]
                + [u_ref[x, h, rows] for h in range(nh)]
                + [hhi[x, r, rows] for r in range(3)]
            )
            fourth, to_up, to_down, pair, middle = column_parts(line, theta_floor)
            up_3 = {j: to_up[j] * 3.0 for j in range(nh)}
            down_3 = {j: to_down[j] * 3.0 for j in range(nh)}
            for h in range(nh):
                term = two_sided(fourth, to_up, to_down, up_3, down_3, pair, middle, h)
                change = dt * jnp.minimum(
                    acc_ref[x, h, rows] + term * (0.5 * TURN_MAX / d_theta), 0.0
                )
                u = line[h + 3]
                if stage == 1:
                    value = u + change
                elif stage == 2:
                    value = 0.75 * base_ref[x, h, rows] + 0.25 * (u + change)
                else:
                    value = (2.0 / 3.0) * ((u - base_ref[x, h, rows]) + change)
                out_ref[x, h, rows] = value
                if stage < 3:
                    if h < 3:
                        faces[2][x, h, rows] = value
                    if h >= nh - 3:
                        faces[3][x, h - nh + 3, rows] = value
        if stage < 3:
            for h in range(nh):
                faces[0][x, h] = out_ref[x, h, pl.ds(mate_row, 3)]
                faces[1][x, h] = out_ref[x, h, pl.ds(ny - 3 - mate_row, 3)]
        else:
            pltpu.make_async_copy(out_ref.at[x], whole_ref.at[x], sent.at[x]).start()
        return carry

    lax.fori_loop(0, nx, along_heading, 0)
    if stage == 3:
        for x in range(nx):
            pltpu.make_async_copy(out_ref.at[x], whole_ref.at[x], sent.at[x]).wait()


def rate_kernel(wind_ref, out_ref, *, spots):
    wind_x = wind_ref[0]
    wind_y = wind_ref[1]
    top = None
    for move_x, move_y in spots:
        fast = jnp.abs(wind_x + move_x) + jnp.abs(wind_y + move_y)
        top = fast if top is None else jnp.maximum(top, fast)
    out_ref[...] = jnp.full(out_ref.shape, jnp.max(top), jnp.float32)


VMEM = pl.BlockSpec(memory_space=pltpu.VMEM)


def body(level_set, wind_field):
    field = jnp.transpose(level_set, (0, 2, 1, 3))
    nx, nh, ny, nv = field.shape
    n_head = nh * lax.axis_size("ha")
    d_theta = 2.0 * math.pi / n_head
    d_speed = SPEED_SPAN / nv
    every_angle = np.arange(n_head, dtype=np.float32) * np.float32(d_theta)
    ends = [SPEED_LOW + SPEED_SPAN * 0.5 / nv, SPEED_LOW + SPEED_SPAN * (nv - 0.5) / nv]
    spots = [
        (float(np.float32(v) * np.cos(angle)), float(np.float32(v) * np.sin(angle)))
        for v in ends
        for angle in every_angle
    ]
    top = pl.pallas_call(
        functools.partial(rate_kernel, spots=spots),
        out_shape=jax.ShapeDtypeStruct((8, 128), jnp.float32),
        in_specs=[VMEM],
        out_specs=VMEM,
        compiler_params=pltpu.CompilerParams(vmem_limit_bytes=4 << 20),
        name="rate",
    )(wind_field)

    speeds = SPEED_LOW + SPEED_SPAN * (jnp.arange(nv, dtype=jnp.float32) + 0.5) / nv
    angles = (lax.axis_index("ha") * nh + jnp.arange(nh, dtype=jnp.int32)).astype(
        jnp.float32
    ) * d_theta
    heading = jnp.stack([jnp.cos(angles), jnp.sin(angles)])
    velocity = heading[:, :, None, None] * jnp.broadcast_to(
        speeds * (0.5 / CELL_SIZE), (2, nh, 8, nv)
    )
    wind = jnp.broadcast_to((wind_field * (0.5 / CELL_SIZE))[..., None], (2, nx, ny, nv))

    shape = jax.ShapeDtypeStruct(field.shape, jnp.float32)
    y_face = jax.ShapeDtypeStruct((nx, nh, 3, nv), jnp.float32)
    h_face = jax.ShapeDtypeStruct((nx, 3, ny, nv), jnp.float32)

    def speed_part(u, share=(0, 1), filled=()):
        flat = (nx * nh * ny, nv)
        count = flat[0] // 128
        return pl.pallas_call(
            functools.partial(
                speed_kernel, d_speed=d_speed, blocks=tuple(int(count * s) for s in share)
            ),
            out_shape=jax.ShapeDtypeStruct(flat, jnp.float32),
            in_specs=[VMEM] * (1 + len(filled)),
            out_specs=VMEM,
            input_output_aliases={1: 0} if filled else {},
            scratch_shapes=[pltpu.VMEM((count, nv + 16, 128), jnp.float32)] * 7,
            cost_estimate=pl.CostEstimate(
                flops=100 * nx * nh * ny * nv, bytes_accessed=8 * nx * nh * ny * nv, transcendentals=0
            ),
            compiler_params=pltpu.CompilerParams(vmem_limit_bytes=12 << 20),
            name="speed",
        )(u.reshape(flat), *(f.reshape(flat) for f in filled)).reshape(u.shape)

    def plane_part(u, part, xlo, xhi, ymate, yother):
        return pl.pallas_call(
            plane_kernel,
            out_shape=shape,
            in_specs=[VMEM] * 8,
            out_specs=VMEM,
            scratch_shapes=[
                pltpu.VMEM((nx, nh, ny + 16, nv), jnp.float32),
                pltpu.VMEM((nx, nh, UP, nv), jnp.float32),
            ],
            cost_estimate=pl.CostEstimate(
                flops=200 * nx * nh * ny * nv, bytes_accessed=16 * nx * nh * ny * nv, transcendentals=0
            ),
            compiler_params=pltpu.CompilerParams(vmem_limit_bytes=24 << 20),
            name="plane",
        )(u, part, xlo, xhi, ymate, yother, velocity, wind)

    def heading_part(stage, u, acc, hlo, hhi):
        outs = [shape]
        if stage < 3:
            outs += [y_face, y_face, h_face, h_face]
        ins = [top, u, acc] + ([field] if stage > 1 else []) + [hlo, hhi]
        return pl.pallas_call(
            functools.partial(heading_kernel, stage=stage, d_theta=d_theta, d_speed=d_speed),
            out_shape=outs,
            in_specs=[VMEM] * len(ins),
            out_specs=[VMEM] * len(outs) if stage < 3 else [pl.BlockSpec(memory_space=pl.ANY)],
            scratch_shapes=(
                []
                if stage < 3
                else [pltpu.VMEM(shape.shape, jnp.float32), pltpu.SemaphoreType.DMA((nx,))]
            ),
            cost_estimate=pl.CostEstimate(
                flops=100 * nx * nh * ny * nv, bytes_accessed=16 * nx * nh * ny * nv, transcendentals=0
            ),
            compiler_params=pltpu.CompilerParams(vmem_limit_bytes=24 << 20),
        )(*ins)

    def exchange(u, y_mate, y_other, h_first, h_last):
        def halo(value, axis, step):
            count = lax.axis_size(axis)
            return lax.ppermute(value, axis, [(i, step(i) % count) for i in range(count)])

        xlo = halo(u[nx - 3 :], "gx", lambda i: i + 1)
        xhi = halo(u[:3], "gx", lambda i: i - 1)
        ymate = halo(y_mate, "gy", lambda i: i ^ 1)
        yother = halo(y_other, "gy", lambda i: i + 1 if i % 2 else i - 1)
        hlo = halo(h_last, "ha", lambda i: i + 1)
        hhi = halo(h_first, "ha", lambda i: i - 1)
        return xlo, xhi, ymate, yother, hlo, hhi

    for axis, bit in [("gx", 1), ("gx", 2), ("gy", 1), ("gy", 2), ("gy", 4)]:
        other = lax.ppermute(top, axis, [(j, j ^ bit) for j in range(lax.axis_size(axis))])
        top = jnp.maximum(top, other)

    even = lax.axis_index("gy") % 2 == 0
    y_first, y_last = field[:, :, :3], field[:, :, ny - 3 :]
    faces = (
        jnp.where(even, y_last, y_first),
        jnp.where(even, y_first, y_last),
        field[:, :3],
        field[:, nh - 3 :],
    )
    u = field
    for stage in (1, 2, 3):
        xlo, xhi, ymate, yother, hlo, hhi = exchange(u, *faces)
        if stage > 1:
            part = speed_part(u)
        else:
            part = speed_part(u, (0, 0.5))
            part = speed_part(u, (0.5, 1), (part,))
        acc = plane_part(u, part, xlo, xhi, ymate, yother)
        u, *faces = heading_part(stage, u, acc, hlo, hhi)
    return jnp.transpose(u, (0, 2, 1, 3))


def solution(mesh):
    return jax.shard_map(
        body,
        mesh=mesh,
        in_specs=(P("gx", "gy", "ha", None), P(None, "gx", "gy")),
        out_specs=P("gx", "gy", "ha", None),
        check_vma=False,
    )
```

```python
import functools
import math

import jax
import jax.numpy as jnp
import numpy as np
from jax import lax
from jax.experimental import pallas as pl
from jax.experimental.pallas import tpu as pltpu
from jax.sharding import PartitionSpec as P


CELL_SIZE = 0.05
SPEED_LOW = 0.1
SPEED_SPAN = 0.4
TURN_MAX = 1.0
ACCEL_MAX = 0.05
CFL_NUMBER = 0.5
WENO_EPS = 1e-06

LEAN = 1.375
LEVEL = 0.625
REST = 0.609375
UP = 24


def floor_of(spacing):
    return 0.75 * WENO_EPS * spacing * spacing


def squared(value):
    return value * value


def inverse_square(value):
    return squared(1.0 / value)


def one_sided(flow, below_two, below, center, above, above_two, across, floor):
    ahead = flow > 0.0
    far = jnp.where(ahead, above_two, below_two)
    near = jnp.where(ahead, above, below)
    back = jnp.where(ahead, below, above)
    near_rest = squared(near) * REST + floor
    center_rest = squared(center) * REST + floor
    weight_one = inverse_square(squared(far - near * LEAN) + near_rest)
    weight_two = inverse_square(squared(near - center * LEVEL) + center_rest) * 6.0
    weight_three = inverse_square(squared(back - center * LEAN) + center_rest) * 3.0
    step = near - center
    fourth_here = (step - (center - back)) * (1.0 / 3.0)
    fourth_near = ((far - near) - step) * (2.0 / 3.0)
    total = weight_one + weight_two + weight_three
    shift = (weight_one * fourth_near + weight_three * fourth_here) / total - 0.5 * fourth_here
    middle = across - (above - below) * (1.0 / 6.0)
    return flow * middle + jnp.abs(flow) * shift


def column_parts(line, floor):
    rise = [line[i + 1] - line[i] for i in range(len(line) - 1)]
    bend = [rise[i + 1] - rise[i] for i in range(len(rise) - 1)]
    turn = [bend[i + 1] - bend[i] for i in range(len(bend) - 1)]
    fourth = [(turn[i + 1] - turn[i]) * (2.0 / 3.0) for i in range(len(turn) - 1)]
    count = len(line) - 6
    at = lambda j: bend[j + 2]
    rest = {j: squared(at(j)) * REST + floor for j in range(-1, count + 1)}
    lean = {j: at(j) * LEAN for j in range(-1, count + 1)}
    to_up = {j: inverse_square(squared(at(j + 1) - lean[j]) + rest[j]) for j in range(0, count + 1)}
    to_down = {j: inverse_square(squared(at(j - 1) - lean[j]) + rest[j]) for j in range(-1, count)}
    pair = {
        j: inverse_square(squared(at(j - 1) - at(j) * LEVEL) + rest[j]) * 6.0
        for j in range(0, count + 1)
    }
    middle = [
        (line[i + 4] - line[i + 2]) - (at(i + 1) - at(i - 1)) * (1.0 / 6.0) for i in range(count)
    ]
    return (lambda j: fourth[j + 1]), to_up, to_down, pair, middle


def two_sided(fourth, to_up, to_down, to_up_3, to_down_3, pair, middle, i):
    half = 0.5 * fourth(i)
    right = (to_up[i + 1] * fourth(i + 1) + to_down_3[i] * half) / (
        to_up[i + 1] + to_down_3[i] + pair[i + 1]
    )
    left = (to_down[i - 1] * fourth(i - 1) + to_up_3[i] * half) / (
        to_down[i - 1] + to_up_3[i] + pair[i]
    )
    return jnp.maximum(right + middle[i], left - middle[i]) - 0.5 * half


def picked(flow, fourth, to_up, to_down, pair, middle, i):
    ahead = flow > 0.0
    weight_one = jnp.where(ahead, to_up[i + 1], to_down[i - 1])
    weight_two = jnp.where(ahead, pair[i + 1], pair[i])
    weight_three = jnp.where(ahead, to_down[i], to_up[i]) * 3.0
    far = jnp.where(ahead, fourth(i + 1), fourth(i - 1))
    half = 0.5 * fourth(i)
    shift = (weight_one * far + weight_three * half) / (
        weight_one + weight_two + weight_three
    ) - 0.5 * half
    return flow * middle[i] + jnp.abs(flow) * shift


def speed_kernel(u_ref, *refs, d_speed, blocks):
    out_ref, turned, done_ref, *scratch = refs[-13:]
    sets = scratch[:5], scratch[5:]
    nv = u_ref.shape[1]
    floor = floor_of(d_speed)
    top = 1.0 / (floor * floor)
    first, last = 8, 8 + nv

    for b in range(*blocks):
        turned[b, first:last] = u_ref[128 * b : 128 * b + 128].T
    if blocks[0] > 0:
        out_ref[0 : 128 * blocks[0]] = refs[0][0 : 128 * blocks[0]]
    zero = jnp.zeros((8, 128), jnp.float32)
    for bent, up_ref, down_ref, pair_ref, fourth_ref in sets:
        for ref in (bent, fourth_ref):
            ref[first - 8 : first] = zero
            ref[last : last + 8] = zero
        down_ref[first - 8 : first] = zero + top
        up_ref[last : last + 8] = zero + top
        pair_ref[last : last + 8] = zero + 6.0 * top
    for b in range(*blocks):
        turned[b, first - 1 : first] = (
            2.0 * turned[b, first : first + 1] - turned[b, first + 1 : first + 2]
        )
        turned[b, last : last + 1] = (
            2.0 * turned[b, last - 1 : last] - turned[b, last - 2 : last - 1]
        )

    def work(b, bent, up_ref, down_ref, pair_ref, fourth_ref):
        for r in range(first, last, 8):
            here = turned[b, r : r + 8]
            bent[r : r + 8] = (turned[b, r + 1 : r + 9] - here) - (here - turned[b, r - 1 : r + 7])
        for r in range(first, last, 8):
            below, bend, above = (bent[r + d : r + d + 8] for d in (-1, 0, 1))
            rest = squared(bend) * REST + floor
            lean = bend * LEAN
            up_ref[r : r + 8] = inverse_square(squared(above - lean) + rest)
            down_ref[r : r + 8] = inverse_square(squared(below - lean) + rest)
            pair_ref[r : r + 8] = inverse_square(squared(below - bend * LEVEL) + rest) * 6.0
            fourth_ref[r : r + 8] = ((above - bend) - (bend - below)) * (2.0 / 3.0)
        for r in range(first, last, 8):
            half = 0.5 * fourth_ref[r : r + 8]
            up_3 = up_ref[r : r + 8] * 3.0
            down_3 = down_ref[r : r + 8] * 3.0
            up_after = up_ref[r + 1 : r + 9]
            down_before = down_ref[r - 1 : r + 7]
            middle = (turned[b, r + 1 : r + 9] - turned[b, r - 1 : r + 7]) - (
                bent[r + 1 : r + 9] - bent[r - 1 : r + 7]
            ) * (1.0 / 6.0)
            right = (up_after * fourth_ref[r + 1 : r + 9] + down_3 * half) / (
                up_after + down_3 + pair_ref[r + 1 : r + 9]
            )
            left = (down_before * fourth_ref[r - 1 : r + 7] + up_3 * half) / (
                down_before + up_3 + pair_ref[r : r + 8]
            )
            done_ref[b, r : r + 8] = (jnp.maximum(right + middle, left - middle) - 0.5 * half) * (
                0.5 * ACCEL_MAX / d_speed
            )

    def two(i, carry):
        b = blocks[0] + 2 * i
        work(b, *sets[0])
        work(b + 1, *sets[1])
        return carry

    lax.fori_loop(0, (blocks[1] - blocks[0]) // 2, two, 0)
    for b in range(*blocks):
        out_ref[128 * b : 128 * b + 128] = done_ref[b, first:last].T


def ghosts(edge, inner):
    slope = edge - inner
    one = edge + slope
    two = one + slope
    return one, two, two + slope


def rows_kernel(
    u_ref, part_ref, ymate, yother, vel_ref, wind_ref, acc_ref, pad_ref, bend_ref
):
    nx, nh, ny, nv = u_ref.shape
    floor = floor_of(CELL_SIZE)
    gy = lax.axis_index("gy")
    at_edge = jnp.logical_or(gy == 0, gy == lax.axis_size("gy") - 1)
    odd = lax.rem(gy, 2)
    mate_at = 8 + ny - odd * (ny + 3)
    other_at = 5 + odd * (ny + 3)
    edge_row = odd * (ny - 1)
    inner_row = 1 + odd * (ny - 3)
    row = lax.broadcasted_iota(jnp.int32, (3, nv), 0)
    reach = (3 - row + odd * (2 * row - 2)).astype(jnp.float32)

    def fill(x, carry):
        for h in range(nh):
            pad_ref[x, h, 8 : 8 + ny] = u_ref[x, h]
            pad_ref[x, h, pl.ds(mate_at, 3)] = ymate[x, h]
            edge = u_ref[x, h, pl.ds(edge_row, 3, stride=0)]
            inner = u_ref[x, h, pl.ds(inner_row, 3, stride=0)]
            pad_ref[x, h, pl.ds(other_at, 3)] = jnp.where(
                at_edge, edge + reach * (edge - inner), yother[x, h]
            )
        for h in range(nh):
            for r in range(0, UP, 8):
                here = pad_ref[x, h, r + 6 : r + 14]
                bend_ref[x, h, r : r + 8] = (pad_ref[x, h, r + 7 : r + 15] - here) - (
                    here - pad_ref[x, h, r + 5 : r + 13]
                )
        return carry

    lax.fori_loop(0, nx, fill, 0)

    def along_y(x, carry):
        for h in range(nh):
            for r in range(0, ny, 8):
                flow = vel_ref[1, h] + wind_ref[1, x, r : r + 8]
                across = pad_ref[x, h, 9 + r : 17 + r] - pad_ref[x, h, 7 + r : 15 + r]
                near = [bend_ref[x, h, r + s : r + s + 8] for s in range(5)]
                acc_ref[x, h, r : r + 8] = part_ref[x, h, r : r + 8] + one_sided(
                    flow, *near, across, floor
                )
        return carry

    lax.fori_loop(0, nx, along_y, 0)


def columns_kernel(u_ref, part_ref, xmate, xother, vel_ref, wind_ref, acc_ref):
    nx, nh, ny, _ = u_ref.shape
    halves = ny // 8
    floor = floor_of(CELL_SIZE)
    gx = lax.axis_index("gx")
    at_x_edge = jnp.logical_or(gx == 0, gx == lax.axis_size("gx") - 1)
    x_even = lax.rem(gx, 2) == 0

    def along_x(h, carry, mate_above):
        for half in range(halves):
            rows = slice(8 * half, 8 * half + 8)
            mine = [u_ref[x, h, rows] for x in range(nx)]
            near = [xmate[r, h, rows] for r in range(3)]
            if mate_above:
                past = ghosts(mine[0], mine[1])[::-1]
            else:
                past = ghosts(mine[nx - 1], mine[nx - 2])
            away = [jnp.where(at_x_edge, past[r], xother[r, h, rows]) for r in range(3)]
            line = away + mine + near if mate_above else near + mine + away
            fourth, to_up, to_down, pair, middle = column_parts(line, floor)
            speed = vel_ref[0, h]
            for x in range(nx):
                flow = speed + wind_ref[0, x, rows]
                acc_ref[x, h, rows] = part_ref[x, h, rows] + picked(
                    flow, fourth, to_up, to_down, pair, middle, x
                )
        return carry

    @pl.when(x_even)
    def _():
        lax.fori_loop(0, nh, functools.partial(along_x, mate_above=True), 0)

    @pl.when(jnp.logical_not(x_even))
    def _():
        lax.fori_loop(0, nh, functools.partial(along_x, mate_above=False), 0)


def heading_kernel(top_ref, u_ref, acc_ref, *refs, stage, d_theta, d_speed):
    refs = list(refs)
    base_ref = refs.pop(0) if stage > 1 else None
    hmate, hother, out_ref, *faces = refs
    if stage == 3:
        whole_ref, out_ref, sent = out_ref, *faces
        faces = None
    nx, nh, ny, _ = u_ref.shape
    halves = ny // 8
    x_even, y_even, h_even = (1 - lax.rem(lax.axis_index(a), 2) for a in ("gx", "gy", "ha"))
    mate_row = y_even * (ny - 3)
    mate_head = h_even * (nh - 3)
    mate_x = x_even * (nx - 3)
    dt = CFL_NUMBER / (
        top_ref[...] * (1.0 / CELL_SIZE) + (TURN_MAX / d_theta + ACCEL_MAX / d_speed)
    )
    theta_floor = floor_of(d_theta)

    def along_heading(x, carry, mate_above):
        hlo, hhi = (hother, hmate) if mate_above else (hmate, hother)
        for half in range(halves):
            rows = slice(8 * half, 8 * half + 8)
            line = (
                [hlo[x, r, rows] for r in range(3)]
                + [u_ref[x, h, rows] for h in range(nh)]
                + [hhi[x, r, rows] for r in range(3)]
            )
            fourth, to_up, to_down, pair, middle = column_parts(line, theta_floor)
            up_3 = {j: to_up[j] * 3.0 for j in range(nh)}
            down_3 = {j: to_down[j] * 3.0 for j in range(nh)}
            for h in range(nh):
                term = two_sided(fourth, to_up, to_down, up_3, down_3, pair, middle, h)
                change = dt * jnp.minimum(
                    acc_ref[x, h, rows] + term * (0.5 * TURN_MAX / d_theta), 0.0
                )
                u = line[h + 3]
                if stage == 1:
                    value = u + change
                elif stage == 2:
                    value = 0.75 * base_ref[x, h, rows] + 0.25 * (u + change)
                else:
                    value = (2.0 / 3.0) * ((u - base_ref[x, h, rows]) + change)
                out_ref[x, h, rows] = value
        if stage < 3:
            for h in range(nh):
                faces[0][x, h] = out_ref[x, h, pl.ds(mate_row, 3)]
                faces[1][x, h] = out_ref[x, h, pl.ds(ny - 3 - mate_row, 3)]
            for r in range(3):
                faces[2][x, r] = out_ref[x, mate_head + r]
                faces[3][x, r] = out_ref[x, nh - 3 - mate_head + r]
        else:
            pltpu.make_async_copy(out_ref.at[x], whole_ref.at[x], sent.at[x]).start()
        return carry

    @pl.when(h_even == 1)
    def _():
        lax.fori_loop(0, nx, functools.partial(along_heading, mate_above=True), 0)

    @pl.when(h_even == 0)
    def _():
        lax.fori_loop(0, nx, functools.partial(along_heading, mate_above=False), 0)

    if stage < 3:
        for r in range(3):
            for h in range(nh):
                faces[4][r, h] = out_ref[mate_x + r, h]
                faces[5][r, h] = out_ref[nx - 3 - mate_x + r, h]
    if stage == 3:
        for x in range(nx):
            pltpu.make_async_copy(out_ref.at[x], whole_ref.at[x], sent.at[x]).wait()


def face_kernel(u_ref, *faces):
    nx, nh, ny, _ = u_ref.shape
    x_even, y_even, h_even = (1 - lax.rem(lax.axis_index(a), 2) for a in ("gx", "gy", "ha"))
    mate_row = y_even * (ny - 3)
    mate_head = h_even * (nh - 3)
    mate_x = x_even * (nx - 3)

    def planes(x, carry):
        for h in range(nh):
            faces[0][x, h] = u_ref[x, h, pl.ds(mate_row, 3)]
            faces[1][x, h] = u_ref[x, h, pl.ds(ny - 3 - mate_row, 3)]
        for r in range(3):
            faces[2][x, r] = u_ref[x, mate_head + r]
            faces[3][x, r] = u_ref[x, nh - 3 - mate_head + r]
        return carry

    lax.fori_loop(0, nx, planes, 0)
    for r in range(3):
        for h in range(nh):
            faces[4][r, h] = u_ref[mate_x + r, h]
            faces[5][r, h] = u_ref[nx - 3 - mate_x + r, h]


def rate_kernel(wind_ref, out_ref, *, spots):
    wind_x = wind_ref[0]
    wind_y = wind_ref[1]
    top = None
    for move_x, move_y in spots:
        fast = jnp.abs(wind_x + move_x) + jnp.abs(wind_y + move_y)
        top = fast if top is None else jnp.maximum(top, fast)
    out_ref[...] = jnp.full(out_ref.shape, jnp.max(top), jnp.float32)


VMEM = pl.BlockSpec(memory_space=pltpu.VMEM)


def body(level_set, wind_field):
    field = jnp.transpose(level_set, (0, 2, 1, 3))
    nx, nh, ny, nv = field.shape
    n_head = nh * lax.axis_size("ha")
    d_theta = 2.0 * math.pi / n_head
    d_speed = SPEED_SPAN / nv
    every_angle = np.arange(n_head, dtype=np.float32) * np.float32(d_theta)
    ends = [SPEED_LOW + SPEED_SPAN * 0.5 / nv, SPEED_LOW + SPEED_SPAN * (nv - 0.5) / nv]
    spots = [
        (float(np.float32(v) * np.cos(angle)), float(np.float32(v) * np.sin(angle)))
        for v in ends
        for angle in every_angle
    ]
    top = pl.pallas_call(
        functools.partial(rate_kernel, spots=spots),
        out_shape=jax.ShapeDtypeStruct((8, 128), jnp.float32),
        in_specs=[VMEM],
        out_specs=VMEM,
        compiler_params=pltpu.CompilerParams(vmem_limit_bytes=4 << 20),
        name="rate",
    )(wind_field)

    speeds = SPEED_LOW + SPEED_SPAN * (jnp.arange(nv, dtype=jnp.float32) + 0.5) / nv
    angles = (lax.axis_index("ha") * nh + jnp.arange(nh, dtype=jnp.int32)).astype(
        jnp.float32
    ) * d_theta
    heading = jnp.stack([jnp.cos(angles), jnp.sin(angles)])
    velocity = heading[:, :, None, None] * jnp.broadcast_to(
        speeds * (0.5 / CELL_SIZE), (2, nh, 8, nv)
    )
    wind = jnp.broadcast_to((wind_field * (0.5 / CELL_SIZE))[..., None], (2, nx, ny, nv))

    shape = jax.ShapeDtypeStruct(field.shape, jnp.float32)
    x_face = jax.ShapeDtypeStruct((3, nh, ny, nv), jnp.float32)
    y_face = jax.ShapeDtypeStruct((nx, nh, 3, nv), jnp.float32)
    h_face = jax.ShapeDtypeStruct((nx, 3, ny, nv), jnp.float32)
    all_faces = [y_face, y_face, h_face, h_face, x_face, x_face]
    faces = pl.pallas_call(
        face_kernel,
        out_shape=all_faces,
        in_specs=[VMEM],
        out_specs=[VMEM] * 6,
        compiler_params=pltpu.CompilerParams(vmem_limit_bytes=8 << 20),
        name="faces",
    )(field)

    def speed_part(u, share=(0, 1), filled=()):
        flat = (nx * nh * ny, nv)
        count = flat[0] // 128
        return pl.pallas_call(
            functools.partial(
                speed_kernel, d_speed=d_speed, blocks=tuple(int(count * s) for s in share)
            ),
            out_shape=jax.ShapeDtypeStruct(flat, jnp.float32),
            in_specs=[VMEM] * (1 + len(filled)),
            out_specs=VMEM,
            scratch_shapes=[pltpu.VMEM((count, nv + 16, 128), jnp.float32)] * 2
            + [pltpu.VMEM((nv + 16, 128), jnp.float32)] * 10,
            cost_estimate=pl.CostEstimate(
                flops=100 * nx * nh * ny * nv, bytes_accessed=8 * nx * nh * ny * nv, transcendentals=0
            ),
            compiler_params=pltpu.CompilerParams(vmem_limit_bytes=12 << 20),
            name="speed",
        )(u.reshape(flat), *(f.reshape(flat) for f in filled)).reshape(u.shape)

    def rows_part(u, part, ymate, yother):
        return pl.pallas_call(
            rows_kernel,
            out_shape=shape,
            in_specs=[VMEM] * 6,
            out_specs=VMEM,
            scratch_shapes=[
                pltpu.VMEM((nx, nh, ny + 16, nv), jnp.float32),
                pltpu.VMEM((nx, nh, UP, nv), jnp.float32),
            ],
            cost_estimate=pl.CostEstimate(
                flops=100 * nx * nh * ny * nv, bytes_accessed=16 * nx * nh * ny * nv, transcendentals=0
            ),
            compiler_params=pltpu.CompilerParams(vmem_limit_bytes=24 << 20),
            name="rows",
        )(u, part, ymate, yother, velocity, wind)

    def columns_part(u, part, xmate, xother):
        return pl.pallas_call(
            columns_kernel,
            out_shape=shape,
            in_specs=[VMEM] * 6,
            out_specs=VMEM,
            cost_estimate=pl.CostEstimate(
                flops=100 * nx * nh * ny * nv, bytes_accessed=16 * nx * nh * ny * nv, transcendentals=0
            ),
            compiler_params=pltpu.CompilerParams(vmem_limit_bytes=24 << 20),
            name="columns",
        )(u, part, xmate, xother, velocity, wind)

    def heading_part(stage, u, acc, hmate, hother):
        outs = [shape]
        if stage < 3:
            outs += all_faces
        ins = [top, u, acc] + ([field] if stage > 1 else []) + [hmate, hother]
        return pl.pallas_call(
            functools.partial(heading_kernel, stage=stage, d_theta=d_theta, d_speed=d_speed),
            out_shape=outs,
            in_specs=[VMEM] * len(ins),
            out_specs=[VMEM] * len(outs) if stage < 3 else [pl.BlockSpec(memory_space=pl.ANY)],
            scratch_shapes=(
                []
                if stage < 3
                else [pltpu.VMEM(shape.shape, jnp.float32), pltpu.SemaphoreType.DMA((nx,))]
            ),
            cost_estimate=pl.CostEstimate(
                flops=100 * nx * nh * ny * nv, bytes_accessed=16 * nx * nh * ny * nv, transcendentals=0
            ),
            compiler_params=pltpu.CompilerParams(vmem_limit_bytes=24 << 20),
        )(*ins)

    def exchange(y_mate, y_other, h_mate, h_other, x_mate, x_other):
        def halo(name, value, axis):
            count = lax.axis_size(axis)
            if name[1] == "a":
                pairs = [(i, i ^ 1) for i in range(count)]
            else:
                pairs = [(i, (i + 1 if i % 2 else i - 1) % count) for i in range(count)]
            return lax.ppermute(value, axis, pairs)

        return (
            halo("xa", x_mate, "gx"),
            halo("xb", x_other, "gx"),
            halo("ya", y_mate, "gy"),
            halo("yb", y_other, "gy"),
            halo("ha", h_mate, "ha"),
            halo("hb", h_other, "ha"),
        )

    for axis, bit in [("gx", 1), ("gx", 2), ("gy", 1), ("gy", 2), ("gy", 4)]:
        other = lax.ppermute(top, axis, [(j, j ^ bit) for j in range(lax.axis_size(axis))])
        top = jnp.maximum(top, other)

    u = field
    for stage in (1, 2, 3):
        xmate, xother, ymate, yother, hmate, hother = exchange(*faces)
        if stage > 1:
            part = speed_part(u)
        else:
            part = speed_part(u, (0, 0.4))
            part = speed_part(u, (0.4, 1), (part,))
        acc = rows_part(u, part, ymate, yother)
        acc = columns_part(u, acc, xmate, xother)
        u, *faces = heading_part(stage, u, acc, hmate, hother)
    return jnp.transpose(u, (0, 2, 1, 3))


def solution(mesh):
    return jax.shard_map(
        body,
        mesh=mesh,
        in_specs=(P("gx", "gy", "ha", None), P(None, "gx", "gy")),
        out_specs=P("gx", "gy", "ha", None),
        check_vma=False,
    )
```
